32 devices in a mesh: batch: 4 (over z), seq: 8 (over y, x, core).
Axes of the slice: x: 2, y: 2, z: 4, core: 2. Of those that a mesh axis runs over, the one named last changes fastest.
Arguments:
- tokens: bfloat16 [10240, 8192], P(('batch', 'seq')), may hold values from -6 to 6
- out_grad: bfloat16 [10240, 8192], P(('batch', 'seq')), may hold values from -0.109375 to 0.109375
- gate_pre: bfloat16 [10240, 768], P(('batch', 'seq')), may hold values from -8 to 8
- up_pre: bfloat16 [10240, 768], P(('batch', 'seq')), may hold values from -6 to 6
- hidden_grad: bfloat16 [10240, 768], P(('batch', 'seq')), may hold values from -0.0625 to 0.0625
Outputs:
- gate_weight_grad: float32 [8192, 768], P(('seq', 'batch'))
- up_weight_grad: float32 [8192, 768], P(('seq', 'batch'))
- down_weight_grad: float32 [8192, 768], P(('seq', 'batch'))
The draws below stay inside these ranges and needn't reach their ends.
All inputs are finite; a program needn't handle non-finite values.
Results may differ from the reference program's by a relative error of at most 0.019.
Values may be sent and summed in bfloat16 or wider, within the bound.
No kernel may reach another device: no remote copies, remote signals or barrier semaphores. Data moves between devices by JAX's collectives and lax.ppermute only.
A program may use at most 192 MiB of HBM per device.

```python
import jax
import jax.numpy as jnp
from jax import lax

D = 8192
FF = 768
TOK_DEV = 320
TOKENS = 10240
N_BATCH = 4
N_SEQ = 8


def strengthened(result, stream_key, source, target, blocks, factor):
    owner, partner = [(jnp.arange(result.shape[position]) // (result.shape[position] // blocks)).reshape([-1 if axis == position else 1 for axis in range(result.ndim)]) for position in (source, target)]
    chosen = jax.random.permutation(stream_key, blocks)[partner]
    strong = (owner == chosen) | (owner == (partner + blocks // 2) % blocks)
    return jnp.where(strong, factor * result, result)


def shard_levels(rng, shape, cuts, smallest, top_value):
    factor_of, own = 1.0, jax.random.fold_in(rng, 6)
    for position, blocks in cuts:
        steps = jnp.exp(jax.random.uniform(jax.random.fold_in(own, position), (blocks,), jnp.float32, smallest / len(cuts), top_value / len(cuts)))
        factor_of = factor_of * jnp.repeat(steps, shape[position] // blocks).reshape([-1 if axis == position else 1 for axis in range(len(shape))])
    return factor_of


def gaussian(own_key, extent, deviation, reach, split=(), kind=jnp.bfloat16):
    array = deviation * jax.random.normal(own_key, extent, jnp.float32)
    if split:
        array = array * shard_levels(own_key, extent, split, -0.22, 0.18)
    return jnp.clip(array, -reach, reach).astype(kind)


def heavy_noise(own_key, extent, width, most, split, heavy, kind=jnp.bfloat16):
    entries = width * jax.random.normal(own_key, extent, jnp.float32)
    if split:
        entries = entries * shard_levels(own_key, extent, split, -0.22, 0.18)
    return jnp.clip(strengthened(entries, jax.random.fold_in(own_key, 3), *heavy), -most, most).astype(kind)


def setup_inputs(seed: int = 0) -> dict:
    key_of = jax.random.split(jax.random.key(seed), 6)
    tokens = heavy_noise(key_of[0], (TOKENS, D), 1.0, 6.0, ((0, 32),), (0, 1, 32, 2.75))
    out_grad = heavy_noise(key_of[1], (TOKENS, D), TOKENS ** -0.5, 0.109375, ((0, 32),), (0, 1, 32, 2.75))
    gate_pre = gaussian(key_of[2], (TOKENS, FF), 1.5, 8.0, ((0, 32),))
    up_pre = gaussian(key_of[3], (TOKENS, FF), 1.0, 6.0, ((0, 32),))
    hidden_grad = gaussian(key_of[4], (TOKENS, FF), TOKENS ** -0.5, 0.0625, ((0, 32),))
    return {"tokens": tokens, "out_grad": out_grad, "gate_pre": gate_pre, "up_pre": up_pre, "hidden_grad": hidden_grad}


def hidden_parts(gate_pre, up_pre, hidden_grad):
    gate_val = gate_pre.astype(jnp.float32)
    up_val = up_pre.astype(jnp.float32)
    grad_val = hidden_grad.astype(jnp.float32)
    sigmoid_val = jax.nn.sigmoid(gate_val)
    activated = gate_val * sigmoid_val
    hidden = (activated * up_val).astype(jnp.bfloat16)
    up_cotangent = (grad_val * activated).astype(jnp.bfloat16)
    gate_cotangent = (grad_val * up_val * sigmoid_val * (1.0 + gate_val * (1.0 - sigmoid_val))).astype(jnp.bfloat16)
    return hidden, gate_cotangent, up_cotangent


def contract_rows(left, right):
    return lax.dot_general(left, right, (((0,), (0,)), ((), ())), preferred_element_type=jnp.float32)


def reference(tokens, out_grad, gate_pre, up_pre, hidden_grad):
    hidden, gate_cotangent, up_cotangent = hidden_parts(gate_pre, up_pre, hidden_grad)
    cotangents = jnp.concatenate([gate_cotangent, up_cotangent], axis=1)
    blocks = N_BATCH * N_SEQ
    model_width = tokens.shape[1]
    hidden_width = hidden.shape[1]

    def add_block(total, pieces):
        features, grads, cotangent_rows, hidden_slice = pieces
        term = jnp.concatenate([contract_rows(features, cotangent_rows), contract_rows(grads, hidden_slice)], axis=1)
        return total + lax.optimization_barrier(term.astype(jnp.bfloat16)).astype(jnp.float32), None

    pieces = (tokens.reshape(blocks, TOK_DEV, model_width), out_grad.reshape(blocks, TOK_DEV, model_width),
              cotangents.reshape(blocks, TOK_DEV, 2 * hidden_width), hidden.reshape(blocks, TOK_DEV, hidden_width))
    total, unused = lax.scan(add_block, jnp.zeros((model_width, 3 * hidden_width), jnp.float32), pieces)
    return (total[:, :hidden_width], total[:, hidden_width:2 * hidden_width], total[:, 2 * hidden_width:])
```

```python
import jax
import jax.numpy as jnp
from jax import lax
from jax.sharding import PartitionSpec as P

BF16 = jnp.bfloat16
F32 = jnp.float32
BATCH_FIRST = 3


def hidden_parts(gate_pre, up_pre, hidden_grad):
    gate_val = gate_pre.astype(F32)
    up_val = up_pre.astype(F32)
    grad_val = hidden_grad.astype(F32)
    sigmoid_val = jax.nn.sigmoid(gate_val)
    activated = gate_val * sigmoid_val
    hidden = (activated * up_val).astype(BF16)
    up_cotangent = (grad_val * activated).astype(BF16)
    gate_cotangent = (
        grad_val * up_val * sigmoid_val * (1.0 + gate_val * (1.0 - sigmoid_val))
    ).astype(BF16)
    return hidden, gate_cotangent, up_cotangent


def contract_rows(left, right):
    return lax.dot_general(
        left, right, (((0,), (0,)), ((), ())), preferred_element_type=F32
    )


def pick(index, choices):
    result = choices[0]
    for number, choice in enumerate(choices[1:], 1):
        result = jnp.where(index == number, choice, result)
    return result


def ring_scatter(blocks, axis, count):
    me = lax.axis_index(axis)
    up = [(i, (i + 1) % count) for i in range(count)]
    down = [(i, (i - 1) % count) for i in range(count)]
    own = blocks(me).astype(F32)
    if count == 1:
        return own
    far = count // 2
    rest = count - far
    width = own.shape[-1]
    cut = width // 2
    if count % 2 == 0:
        block = blocks((me + far) % count).astype(F32)
        forward = block[..., :cut]
        backward = block[..., cut:]
        got_up = lax.ppermute(forward.astype(BF16), axis, up).astype(F32)
        got_down = lax.ppermute(backward.astype(BF16), axis, down).astype(F32)
        for step in range(far - 1, 0, -1):
            ahead = blocks((me + step) % count).astype(F32)
            behind = blocks((me - step) % count).astype(F32)
            if got_up.shape[-1] != width:
                ahead = jnp.concatenate([ahead[..., :cut] + got_up, ahead[..., cut:]], axis=-1)
                behind = jnp.concatenate([behind[..., :cut], behind[..., cut:] + got_down], axis=-1)
            else:
                ahead = ahead + got_up
                behind = behind + got_down
            got_up = lax.ppermute(ahead.astype(BF16), axis, up).astype(F32)
            got_down = lax.ppermute(behind.astype(BF16), axis, down).astype(F32)
        if got_up.shape[-1] != width:
            return own + jnp.concatenate([got_up, got_down], axis=-1)
        return own + got_up + got_down
    total = own
    for step in range(1, rest + far):
        sent = blocks((me + step) % count).astype(BF16)
        perm = [(i, (i + step) % count) for i in range(count)]
        total = total + lax.ppermute(sent, axis, perm).astype(F32)
    return total


def make_on_device(count_batch, count_seq):
    count_hi = count_seq // 4

    def moved(by_hi, by_mid, by_core):
        return [
            (i, ((i // 4 + by_hi) % count_hi) * 4 + ((i % 4) ^ (2 * by_mid + by_core)))
            for i in range(count_seq)
        ]

    near = moved(0, 0, 1)

    def on_device(tokens, out_grad, gate_pre, up_pre, hidden_grad):
        seq = lax.axis_index("seq")
        core = seq % 2
        mid = (seq // 2) % 2
        hi = seq // 4
        hidden, gate_cot, up_cot = hidden_parts(gate_pre, up_pre, hidden_grad)
        ff = hidden.shape[1]
        model = tokens.shape[1]
        stripe = model // count_seq
        block = stripe // count_batch
        half = block // 2

        sizes = (2, count_hi)
        places = (mid, hi)

        def step_of(axis, step, by_core=0):
            return moved(0, step, by_core) if axis == 0 else moved(step, 0, by_core)

        cots = jnp.concatenate([gate_cot, up_cot], axis=1)
        cots_of = []
        for axis in range(2):
            straight = [cots] + [
                lax.ppermute(cots, "seq", step_of(axis, step)) for step in range(1, sizes[axis])
            ]
            cots_of.append(straight)

        grads_by_core = [
            jnp.concatenate(
                [out_grad[:, (2 * k + c) * stripe : (2 * k + c + 1) * stripe] for k in range(count_seq // 2)],
                axis=1,
            )
            for c in range(2)
        ]
        grads_near = lax.ppermute(pick(1 - core, grads_by_core), "seq", near)
        hidden_near = lax.ppermute(hidden, "seq", near)
        grads_pair = jnp.concatenate([pick(core, grads_by_core), grads_near], axis=0)
        hidden_pair = jnp.concatenate([hidden, hidden_near], axis=0)

        cut = ff * BATCH_FIRST // 6
        first = contract_rows(grads_pair, hidden_pair[:, :cut]).astype(BF16)
        first = first.reshape(count_seq // 2, count_batch, block, cut)
        late_tokens, first = lax.optimization_barrier((tokens, first))

        def half_columns(source, index, axis):
            start = index * stripe + axis * half
            return jnp.concatenate(
                [source[:, start + z * block : start + z * block + half] for z in range(count_batch)],
                axis=1,
            )

        def gather(source, axis, scatter_place):
            pieces = []
            for step in range(sizes[axis]):
                for by_core in range(2):
                    gather_place = (places[axis] + step) % sizes[axis]
                    place_mid, place_hi = (
                        (gather_place, scatter_place) if axis == 0 else (scatter_place, gather_place)
                    )
                    place_core = core if by_core == 0 else 1 - core
                    piece = pick(
                        place_hi,
                        [
                            pick(
                                place_mid,
                                [
                                    pick(
                                        place_core,
                                        [half_columns(source, 4 * h + 2 * m + c, axis) for c in range(2)],
                                    )
                                    for m in range(2)
                                ],
                            )
                            for h in range(count_hi)
                        ],
                    )
                    if step or by_core:
                        piece = lax.ppermute(piece, "seq", step_of(axis, step, by_core))
                    pieces.append(piece)
            return jnp.concatenate(pieces, axis=0)

        gathered_of = [
            [
                gather(tokens if step else late_tokens, axis, (places[1 - axis] + step) % sizes[1 - axis])
                for step in list(range(1, sizes[1 - axis])) + [0]
            ]
            for axis in range(2)
        ]

        def over_seq(rows):
            total = lax.dynamic_index_in_dim(rows, hi, 0, keepdims=False).astype(F32)
            for step in range(1, count_hi):
                sent = lax.dynamic_index_in_dim(rows, (hi + step) % count_hi, 0, keepdims=False)
                got = lax.ppermute(sent.astype(BF16), "seq", moved(step, 0, 0))
                total = total + got.astype(F32)
            sent = pick(1 - mid, [total[0], total[1]]).astype(BF16)
            return pick(mid, [total[0], total[1]]) + lax.ppermute(
                sent, "seq", moved(0, 1, 0)
            ).astype(F32)

        first = ring_scatter(
            lambda z: lax.dynamic_index_in_dim(first, z, 1, keepdims=False), "batch", count_batch
        )
        down_outs = [over_seq(first.reshape(count_hi, 2, block, cut))]
        if cut < ff:
            second = contract_rows(grads_pair, hidden_pair[:, cut:]).astype(BF16)
            second = over_seq(second.reshape(count_hi, 2, stripe, ff - cut)).astype(BF16)
            second = second.reshape(count_batch, block, ff - cut)

        cots_full = []
        for axis in range(2):
            pieces = []
            for straight in cots_of[axis]:
                pieces.append(straight)
                pieces.append(
                    cots_near if straight is cots and axis else lax.ppermute(straight, "seq", near)
                )
                if straight is cots and not axis:
                    cots_near = pieces[-1]
            cots_full.append(jnp.concatenate(pieces, axis=0))

        outs = []
        for part in range(2):
            halves = []
            for axis in range(2):
                cot = cots_full[axis][:, part * ff : (part + 1) * ff]
                parts = gathered_of[axis]
                received = [
                    lax.ppermute(
                        contract_rows(parts[step - 1], cot).astype(BF16),
                        "seq",
                        step_of(1 - axis, step),
                    )
                    for step in range(1, sizes[1 - axis])
                ]
                kept = contract_rows(parts[-1], cot)
                for piece in received:
                    kept = kept + piece.astype(F32)
                halves.append(kept.astype(BF16).reshape(count_batch, half, ff))
            both = jnp.concatenate(halves, axis=1)
            outs.append(
                ring_scatter(
                    lambda z, both=both: lax.dynamic_index_in_dim(both, z, 0, keepdims=False),
                    "batch",
                    count_batch,
                )
            )
        if cut < ff:
            down_outs.append(
                ring_scatter(
                    lambda z: lax.dynamic_index_in_dim(second, z, 0, keepdims=False),
                    "batch",
                    count_batch,
                )
            )
        return (
            outs[0],
            outs[1],
            jnp.concatenate(down_outs, axis=1) if cut < ff else down_outs[0],
        )

    return on_device


def solution(mesh):
    rows = P(("batch", "seq"), None)
    outs = P(("seq", "batch"), None)
    return jax.shard_map(
        make_on_device(mesh.shape["batch"], mesh.shape["seq"]),
        mesh=mesh,
        in_specs=(rows,) * 5,
        out_specs=(outs,) * 3,
        check_vma=False,
    )
```
